32 devices in a mesh: seq: 8 (over y, x, core), state: 4 (over z).
Axes of the slice: x: 2, y: 2, z: 4, core: 2. Of those that a mesh axis runs over, the one named last changes fastest.
Arguments:
- inputs: bfloat16 [4096, 2048], P('seq', 'state'), may hold values from -6 to 6
- out_grad: bfloat16 [4096, 2048], P('seq', 'state'), may hold values from -6 to 6
- in_proj: bfloat16 [2048, 2048], P('state'), may hold values from -0.125 to 0.125
- out_proj: bfloat16 [2048, 2048], P(None, 'state'), may hold values from -0.125 to 0.125
- rates: float32 [2048], P('state'), may hold values from 4.8828126e-05 to 0.03
- time_step: float32 [4096], P('seq'), may hold values from 0.5 to 16384, as said below
Outputs:
- grad_inputs: bfloat16 [4096, 2048], P('seq', 'state')
- grad_in_proj: float32 [2048, 2048], P('state')
- grad_out_proj: float32 [2048, 2048], P(None, 'state')
- grad_rates: float32 [2048], P('state')
The draws below stay inside these ranges and needn't reach their ends.
Inputs may be any that keep to these rules, and one draw needn't show every extreme that they name: `time_step`: positive time steps.
All inputs are finite; a program needn't handle non-finite values.
Results may differ from the reference program's by a relative error of at most 0.017.
Values may be sent and summed in bfloat16 or wider, within the bound.
A program may use at most 64 MiB of HBM per device.

```python
import math
import jax
import jax.numpy as jnp
from jax import lax

H = 2048
N = 2048
SPAN_LENGTH = 4096
N_STATE = 4


def draw_time_step(key, part):
    first = jax.random.fold_in(key, 11)
    second = jax.random.fold_in(key, 12)
    final_segment = jax.random.fold_in(key, 13)
    starting_index = jnp.exp(jax.random.uniform(first, (SPAN_LENGTH,), jnp.float32, jnp.log(0.5), jnp.log(2.0)))
    location_indices = jax.random.randint(second, (8,), 0, SPAN_LENGTH)
    clustered_batches = jax.random.uniform(final_segment, (8,), jnp.float32, 0.125, 0.35) * (10.0 * SPAN_LENGTH)
    return starting_index.at[location_indices].set(clustered_batches)


def block_levels(key, dims, shards, low, largest):
    level, own = 1.0, jax.random.fold_in(key, 6)
    for dim, shards_of in shards:
        draws = jnp.exp(jax.random.uniform(jax.random.fold_in(own, dim), (shards_of,), jnp.float32, low / len(shards), largest / len(shards)))
        level = level * jnp.repeat(draws, dims[dim] // shards_of).reshape([-1 if axis == dim else 1 for axis in range(len(dims))])
    return level


def noise(key, shape, spread, bound, shards=(), dtype=jnp.bfloat16):
    array = spread * jax.random.normal(key, shape, jnp.float32)
    if shards:
        array = array * block_levels(key, shape, shards, -0.22, 0.18)
    return jnp.clip(array, -bound, bound).astype(dtype)


def setup_inputs(seed: int = 0) -> dict:
    key_list = jax.random.split(jax.random.key(seed), 7)
    inputs = noise(key_list[0], (SPAN_LENGTH, H), 1.0, 6.0, ((0, 8), (1, 4)))
    out_grad = noise(key_list[1], (SPAN_LENGTH, H), 1.0, 6.0, ((0, 8), (1, 4)))
    in_proj = noise(key_list[2], (N, H), H ** -0.5, 0.125, ((0, 4),))
    out_proj = noise(key_list[3], (H, N), N ** -0.5, 0.125, ((1, 4),))
    rates = jnp.clip(jnp.exp(math.log(0.03) - 6.420646 * jax.random.uniform(key_list[4], (N,), jnp.float32) ** block_levels(key_list[4], (N,), ((0, 4),), -0.2, 0.2)), 4.882812572759576e-05, 0.03)
    time_step = draw_time_step(jax.random.fold_in(key_list[6], 71), 0)
    return dict(inputs=inputs, out_grad=out_grad, in_proj=in_proj, out_proj=out_proj, rates=rates, time_step=time_step)


def combine(earlier, later):
    return (earlier[0] * later[0], later[0] * earlier[1] + later[1])


def reference(inputs, out_grad, in_proj, out_proj, rates, time_step):
    decay = jnp.exp(-time_step[:, None] * rates[None, :])
    drive = lax.dot_general(inputs, in_proj, (((1,), (1,)), ((), ())), preferred_element_type=jnp.float32)
    adjoint_in = jnp.dot(out_grad, out_proj, preferred_element_type=jnp.float32)
    states = lax.associative_scan(combine, (decay, drive), axis=0)[1]
    coefs = jnp.concatenate([decay[1:], jnp.zeros((1, decay.shape[1]), jnp.float32)], axis=0)
    flipped = lax.associative_scan(combine, (coefs[::-1], adjoint_in[::-1]), axis=0)[1]
    adjoint = flipped[::-1]
    states_half = states.astype(jnp.bfloat16)
    adjoint_half = adjoint.astype(jnp.bfloat16)
    before = jnp.concatenate([jnp.zeros((1, states.shape[1]), jnp.float32), states[:-1]], axis=0)
    grad_rates = -jnp.sum(time_step[:, None] * decay * adjoint * before, axis=0)
    grad_in_proj = lax.dot_general(adjoint_half, inputs, (((0,), (0,)), ((), ())), preferred_element_type=jnp.float32)
    grad_out_proj = lax.dot_general(out_grad, states_half, (((0,), (0,)), ((), ())), preferred_element_type=jnp.float32)
    width = N // N_STATE

    def add_block(index, total):
        start = (index * width).astype(jnp.int32)
        part_adj = lax.dynamic_slice_in_dim(adjoint_half, start, width, 1)
        part_proj = lax.dynamic_slice_in_dim(in_proj, start, width, 0)
        partial_sum = jnp.dot(part_adj, part_proj, preferred_element_type=jnp.float32)
        return total + partial_sum.astype(jnp.bfloat16).astype(jnp.float32)

    total = lax.fori_loop(0, N_STATE, add_block, jnp.zeros((adjoint.shape[0], in_proj.shape[1]), jnp.float32))
    return total.astype(jnp.bfloat16), grad_in_proj, grad_out_proj, grad_rates
```

```python
import functools

import jax
import jax.numpy as jnp
from jax import lax
from jax.experimental import pallas as pl
from jax.experimental.pallas import tpu as pltpu
from jax.sharding import PartitionSpec as P

MESH = pl.DeviceIdType.MESH
F32, BF16 = jnp.float32, jnp.bfloat16
LANES = 128
SEGMENTS = 8


def remote(src, dst, send, recv, axis, peer):
    return pltpu.make_async_remote_copy(
        src_ref=src,
        dst_ref=dst,
        send_sem=send,
        recv_sem=recv,
        device_id={axis: peer},
        device_id_type=MESH,
    )


def multiple(value, of):
    return pl.multiple_of(value, of)


class Reducer:
    def __init__(self, n, bits, acc, send, recv, full, sems):
        self.n, self.bits, self.acc = n, bits, acc
        self.send, self.recv, self.full = send, recv, full
        self.rs_send, self.rs_recv, self.ag_send, self.ag_recv = sems
        self.rows, self.cols = send.shape[1:]
        self.across = acc.shape[1] // self.cols
        self.me = lax.axis_index("seq")
        self.starts, self.copies, self.spread = [0], [], []
        self.length, self.offset = n, 0

    def part(self, chunk):
        down, over = chunk // self.across, chunk % self.across
        return (
            pl.ds(multiple(down * self.rows, self.rows), self.rows),
            pl.ds(multiple(over * self.cols, self.cols), self.cols),
        )

    def bit(self, b):
        return (self.me // (1 << b)) % 2

    def peer(self, b):
        return self.me + (1 - 2 * self.bit(b)) * (1 << b)

    def start_halving(self, p):
        b, half = self.bits[p], self.length // 2
        start = self.starts[-1]
        away = start + (1 - self.bit(b)) * half
        offset = self.offset

        @pl.loop(0, half)
        def _(c):
            self.send[offset + c] = self.acc[self.part(away + c)].astype(BF16)

        copy = remote(
            self.send.at[pl.ds(offset, half)],
            self.recv.at[pl.ds(offset, half)],
            self.rs_send.at[p],
            self.rs_recv.at[p],
            "seq",
            self.peer(b),
        )
        copy.start()
        self.copies.append(copy)
        self.starts.append(start + self.bit(b) * half)
        self.length, self.offset = half, offset + half

    def end_halving(self, p):
        self.copies[p].wait()
        half, offset, start = self.length, self.offset - self.length, self.starts[-1]

        @pl.loop(0, half)
        def _(c):
            rows = self.part(start + c)
            self.acc[rows] = self.acc[rows] + self.recv[offset + c].astype(F32)

    def finish_own(self):
        start = self.starts[-1]
        self.full[start] = self.acc[self.part(start)].astype(BF16)

    def start_doubling(self, p):
        window = pl.ds(self.starts[p + 1], self.length)
        copy = remote(
            self.full.at[window],
            self.full.at[window],
            self.ag_send.at[p],
            self.ag_recv.at[p],
            "seq",
            self.peer(self.bits[p]),
        )
        copy.start()
        self.spread.append(copy)
        self.length *= 2

    def end_doubling(self):
        self.spread[-1].wait()

    def write(self):
        @pl.loop(0, self.n)
        def _(c):
            self.acc[self.part(c)] = self.full[c].astype(F32)


def kernel(
    n_seq, n_state, bits,
    x_ref, g_ref, b_ref, c_ref, rates_ref, ts_ref,
    gx_ref, gin_ref, gout_ref, gr_ref,
    xg, gg, gt, dec, tsb, dr, ad, bef, h_init, u_init, sh, ah, at,
    car, rbuf, zs, zr,
    in_send, in_recv, in_full, out_send, out_recv, out_full,
    x_sems, g_sems, car_sems, rate_sems, z_sems, bar_sems, bar2_sems,
):
    tokens, feats = x_ref.shape
    chans = b_ref.shape[0]
    tiles, seg = chans // LANES, tokens // SEGMENTS
    seq, state = lax.axis_index("seq"), lax.axis_index("state")

    barrier = pltpu.get_barrier_semaphore()
    for k in range(1, n_seq):
        pl.semaphore_signal(
            barrier, inc=1, device_id={"seq": (seq + k) % n_seq}, device_id_type=MESH
        )
    for k in range(1, n_state):
        pl.semaphore_signal(
            barrier, inc=1, device_id={"state": (state + k) % n_state}, device_id_type=MESH
        )
    pl.semaphore_wait(barrier, n_seq + n_state - 2)

    right, left = (state + 1) % n_state, (state + n_state - 1) % n_state

    def x_block(s):
        return x_ref if s == 0 else xg.at[s - 1]

    def g_block(s):
        return g_ref if s == 0 else gg.at[s - 1]

    def x_columns(s):
        return pl.ds(multiple(((state + n_state - s) % n_state) * feats, feats), feats)

    def g_columns(s):
        return pl.ds(multiple(((state + s) % n_state) * feats, feats), feats)

    def lanes(c):
        return slice(c * LANES, (c + 1) * LANES)

    tm = 256
    for s in range(n_state):
        copies = []
        if s < n_state - 1:
            copies = [
                remote(x_block(s), xg.at[s], x_sems.at[0, s], x_sems.at[1, s], "state", right),
                remote(g_block(s), gg.at[s], g_sems.at[0, s], g_sems.at[1, s], "state", left),
            ]
            for copy in copies:
                copy.start()
        if s == 0:

            @pl.loop(0, tokens // 64)
            def _(r):
                rows = pl.ds(multiple(r * 64, 64), 64)
                step = jnp.broadcast_to(ts_ref[rows, :], (64, LANES))
                tsb[rows, :] = step
                for c in range(tiles):
                    dec[c, rows, :] = jnp.exp(-step * rates_ref[:, lanes(c)])

        xb, gb, xc, gc = x_block(s), g_block(s), x_columns(s), g_columns(s)

        @pl.loop(0, tokens // tm)
        def _(r):
            rows = pl.ds(multiple(r * tm, tm), tm)
            drive = lax.dot_general(
                xb[rows, :], b_ref[:, xc], (((1,), (1,)), ((), ())), preferred_element_type=F32
            )
            for c in range(tiles):
                dr[c, rows, :] = drive[:, lanes(c)] + (0.0 if s == 0 else dr[c, rows, :])
            back = jnp.dot(gb[rows, :], c_ref[gc, :], preferred_element_type=F32)
            for c in range(tiles):
                ad[c, rows, :] = back[:, lanes(c)] + (0.0 if s == 0 else ad[c, rows, :])
            gt[gc, rows] = gb[rows, :].T

        for copy in copies:
            copy.wait()

    def strided(i):
        return pl.ds(i, SEGMENTS, stride=seg)

    zero = jnp.zeros((SEGMENTS, LANES), F32)
    one = jnp.ones((SEGMENTS, LANES), F32)

    def summarise(i, carry):
        hs, ps, us = [], [], []
        j = seg - 1 - i
        for c in range(tiles):
            h, p, u = carry[0][c], carry[1][c], carry[2][c]
            a = dec[c, strided(i), :]
            hs.append(a * h + dr[c, strided(i), :])
            ps.append(a * p)
            us.append(dec[c, strided(j), :] * (u + ad[c, strided(j), :]))
        return tuple(hs), tuple(ps), tuple(us)

    hs, ps, us = lax.fori_loop(
        0, seg, summarise, ((zero,) * tiles, (one,) * tiles, (zero,) * tiles), unroll=4
    )
    for c in range(tiles):
        p, h, u = ps[c][0:1], hs[c][0:1], us[c][SEGMENTS - 1 : SEGMENTS]
        for k in range(1, SEGMENTS):
            h = ps[c][k : k + 1] * h + hs[c][k : k + 1]
            p = p * ps[c][k : k + 1]
            m = SEGMENTS - 1 - k
            u = ps[c][m : m + 1] * u + us[c][m : m + 1]
        car[seq, 0:1, lanes(c)] = p
        car[seq, 1:2, lanes(c)] = h
        car[seq, 2:3, lanes(c)] = u
        car[seq, 3:8, lanes(c)] = jnp.zeros((5, LANES), F32)

    def broadcast(buf, sems):
        copies = []
        for k in range(1, n_seq):
            copy = remote(
                buf.at[seq], buf.at[seq], sems.at[0, k], sems.at[1, k], "seq", (seq + k) % n_seq
            )
            copy.start()
            copies.append(copy)
        return copies

    def collect(buf, sems, copies):
        for k in range(1, n_seq):
            origin = (seq + n_seq - k) % n_seq
            remote(
                buf.at[origin], buf.at[origin], sems.at[0, k], sems.at[1, k], "seq", origin
            ).wait_recv()
        for copy in copies:
            copy.wait_send()

    collect(car, car_sems, broadcast(car, car_sems))
    for c in range(tiles):
        h, u = jnp.zeros((1, LANES), F32), jnp.zeros((1, LANES), F32)
        for k in range(n_seq - 1):
            new = car[k, 0:1, lanes(c)] * h + car[k, 1:2, lanes(c)]
            h = jnp.where(seq > k, new, h)
        for k in range(n_seq - 1, 0, -1):
            new = car[k, 0:1, lanes(c)] * u + car[k, 2:3, lanes(c)]
            u = jnp.where(seq < k, new, u)
        for k in range(SEGMENTS):
            h_init[c, k : k + 1, :] = h
            h = ps[c][k : k + 1] * h + hs[c][k : k + 1]
            m = SEGMENTS - 1 - k
            u_init[c, m : m + 1, :] = u
            u = ps[c][m : m + 1] * u + us[c][m : m + 1]

    def sweep(i, carry):
        hs, us, rs = [], [], []
        for c in range(tiles):
            h = carry[c]
            bef[c, strided(i), :] = h
            h = dec[c, strided(i), :] * h + dr[c, strided(i), :]
            dr[c, strided(i), :] = h
            hs.append(h)
        return tuple(hs)

    lax.fori_loop(0, seg, sweep, tuple(h_init[c] for c in range(tiles)), unroll=4)

    def sweep_back(i, carry):
        us, rs = [], []
        j = seg - 1 - i
        step = tsb[strided(j), :]
        for c in range(tiles):
            adj = ad[c, strided(j), :] + carry[0][c]
            ad[c, strided(j), :] = adj
            u = dec[c, strided(j), :] * adj
            us.append(u)
            rs.append(carry[1][c] + step * u * bef[c, strided(j), :])
        return tuple(us), tuple(rs)

    _, rs = lax.fori_loop(
        0, seg, sweep_back,
        (tuple(u_init[c] for c in range(tiles)), (zero,) * tiles),
        unroll=4,
    )
    for c in range(tiles):
        rbuf[seq, :, lanes(c)] = jnp.broadcast_to(
            -jnp.sum(rs[c], axis=0, keepdims=True), (SEGMENTS, LANES)
        )
    rate_copies = broadcast(rbuf, rate_sems)

    @pl.loop(0, tokens // LANES)
    def _(r):
        rows = pl.ds(multiple(r * LANES, LANES), LANES)
        for c in range(tiles):
            sh[rows, lanes(c)] = dr[c, rows, :].astype(BF16)
            half = ad[c, rows, :].astype(BF16)
            ah[rows, lanes(c)] = half
            at[lanes(c), rows] = half.T

    def input_terms(k):
        cols = pl.ds(multiple(((state + k) % n_state) * feats, feats), feats)

        @pl.loop(0, tokens // tm)
        def _(r):
            rows = pl.ds(multiple(r * tm, tm), tm)
            zs[k, rows, :] = jnp.dot(
                ah[rows, :], b_ref[:, cols], preferred_element_type=F32
            ).astype(BF16)

    z_copies = []
    for k in range(1, n_state):
        input_terms(k)
        copy = remote(
            zs.at[k], zr.at[k], z_sems.at[0, k], z_sems.at[1, k], "state", (state + k) % n_state
        )
        copy.start()
        z_copies.append(copy)

    @pl.loop(0, gt.shape[0] // tm)
    def _(r):
        rows = pl.ds(multiple(r * tm, tm), tm)
        gout_ref[rows, :] = jnp.dot(gt[rows, :], sh[...], preferred_element_type=F32)

    swapped = bits[:1] + bits[:0:-1]
    second = Reducer(
        n_seq, swapped, gout_ref, out_send, out_recv, out_full, [bar2_sems.at[i] for i in range(4)]
    )
    second.start_halving(0)

    for s in range(n_state):
        xb, xc = x_block(s), x_columns(s)

        tc = min(tm, chans)

        @pl.loop(0, chans // tc)
        def _(r):
            rows = pl.ds(multiple(r * tc, tc), tc)
            gin_ref[rows, xc] = jnp.dot(at[rows, :], xb[...], preferred_element_type=F32)

    first = Reducer(
        n_seq, bits, gin_ref, in_send, in_recv, in_full, [bar_sems.at[i] for i in range(4)]
    )
    first.start_halving(0)
    both = (second, first)
    input_terms(0)
    for p in range(len(bits)):
        for red in both:
            red.end_halving(p)
            if p + 1 < len(bits):
                red.start_halving(p + 1)
            else:
                red.finish_own()
                red.start_doubling(p)
    for p in range(len(bits) - 2, -1, -1):
        for red in both:
            red.end_doubling()
            red.start_doubling(p)
        if p == min(1, len(bits) - 2):
            collect(rbuf, rate_sems, rate_copies)
            total = rbuf[0, 0:1, :]
            for k in range(1, n_seq):
                total = total + rbuf[k, 0:1, :]
            gr_ref[...] = total
            for copy in z_copies:
                copy.wait()

            @pl.loop(0, tokens // 64)
            def _(r):
                rows = pl.ds(multiple(r * 64, 64), 64)
                terms = zs[0, rows, :].astype(F32)
                for k in range(1, n_state):
                    terms = terms + zr[k, rows, :].astype(F32)
                gx_ref[rows, :] = terms.astype(BF16)

    for red in both:
        red.end_doubling()
        red.write()


def on_device(inputs, out_grad, in_proj, out_proj, rates, time_step):
    n_seq, n_state = lax.axis_size("seq"), lax.axis_size("state")
    tokens, feats = inputs.shape
    chans, width = in_proj.shape
    tiles = chans // LANES
    bits = list(range(n_seq.bit_length() - 1))
    vmem = pltpu.VMEM
    dma = pltpu.SemaphoreType.DMA
    tile = vmem((tiles, tokens, LANES), F32)
    down = min(n_seq, chans // 16)
    in_part = vmem((n_seq, chans // down, width * down // n_seq), BF16)
    out_part = vmem((n_seq, width // n_seq, chans), BF16)
    whole = pl.BlockSpec(memory_space=pltpu.VMEM)
    gx, gin, gout, gr = pl.pallas_call(
        functools.partial(kernel, n_seq, n_state, bits),
        out_shape=(
            jax.ShapeDtypeStruct((tokens, feats), BF16),
            jax.ShapeDtypeStruct((chans, width), F32),
            jax.ShapeDtypeStruct((width, chans), F32),
            jax.ShapeDtypeStruct((1, chans), F32),
        ),
        in_specs=[whole] * 6,
        out_specs=(whole,) * 4,
        scratch_shapes=[
            vmem((n_state - 1, tokens, feats), BF16),
            vmem((n_state - 1, tokens, feats), BF16),
            vmem((width, tokens), BF16),
            tile,
            vmem((tokens, LANES), F32),
            tile,
            tile,
            tile,
            vmem((tiles, SEGMENTS, LANES), F32),
            vmem((tiles, SEGMENTS, LANES), F32),
            vmem((tokens, chans), BF16),
            vmem((tokens, chans), BF16),
            vmem((chans, tokens), BF16),
            vmem((n_seq, SEGMENTS, chans), F32),
            vmem((n_seq, SEGMENTS, chans), F32),
            vmem((n_state, tokens, feats), BF16),
            vmem((n_state, tokens, feats), BF16),
            in_part, in_part, in_part,
            out_part, out_part, out_part,
            dma((2, n_state)),
            dma((2, n_state)),
            dma((2, n_seq)),
            dma((2, n_seq)),
            dma((2, n_state)),
            dma((4, len(bits))),
            dma((4, len(bits))),
        ],
        compiler_params=pltpu.CompilerParams(
            collective_id=0, has_side_effects=True, vmem_limit_bytes=60 * 1024 * 1024
        ),
    )(
        inputs, out_grad, in_proj, out_proj,
        rates.reshape(1, chans), time_step.reshape(tokens, 1),
    )
    return gx, gin, gout, gr.reshape(chans)


def solution(mesh):
    placed = (
        P("seq", "state"),
        P("seq", "state"),
        P("state", None),
        P(None, "state"),
        P("state"),
        P("seq"),
    )
    return jax.shard_map(
        on_device,
        mesh=mesh,
        in_specs=placed,
        out_specs=(P("seq", "state"), P("state", None), P(None, "state"), P("state")),
        check_vma=False,
    )
```

```python
import functools

import jax
import jax.numpy as jnp
from jax import lax
from jax.experimental import pallas as pl
from jax.experimental.pallas import tpu as pltpu
from jax.sharding import PartitionSpec as P

MESH = pl.DeviceIdType.MESH
F32, BF16 = jnp.float32, jnp.bfloat16
LANES = 128
SEGMENTS = 8


def remote(src, dst, send, recv, axis, peer):
    return pltpu.make_async_remote_copy(
        src_ref=src,
        dst_ref=dst,
        send_sem=send,
        recv_sem=recv,
        device_id={axis: peer},
        device_id_type=MESH,
    )


def multiple(value, of):
    return pl.multiple_of(value, of)


class Reducer:
    def __init__(self, n, bits, acc, send, recv, full, sems):
        self.n, self.bits, self.acc = n, bits, acc
        self.send, self.recv, self.full = send, recv, full
        self.rs_send, self.rs_recv, self.ag_send, self.ag_recv = sems
        self.rows, self.cols = send.shape[1:]
        self.across = acc.shape[1] // self.cols
        self.me = lax.axis_index("seq")
        self.starts, self.copies, self.spread = [0], [], []
        self.length, self.offset = n, 0

    def part(self, chunk):
        down, over = chunk // self.across, chunk % self.across
        return (
            pl.ds(multiple(down * self.rows, self.rows), self.rows),
            pl.ds(multiple(over * self.cols, self.cols), self.cols),
        )

    def bit(self, b):
        return (self.me // (1 << b)) % 2

    def peer(self, b):
        return self.me + (1 - 2 * self.bit(b)) * (1 << b)

    def start_halving(self, p):
        b, half = self.bits[p], self.length // 2
        start = self.starts[-1]
        away = start + (1 - self.bit(b)) * half
        offset = self.offset

        @pl.loop(0, half)
        def _(c):
            self.send[offset + c] = self.acc[self.part(away + c)].astype(BF16)

        copy = remote(
            self.send.at[pl.ds(offset, half)],
            self.recv.at[pl.ds(offset, half)],
            self.rs_send.at[p],
            self.rs_recv.at[p],
            "seq",
            self.peer(b),
        )
        copy.start()
        self.copies.append(copy)
        self.starts.append(start + self.bit(b) * half)
        self.length, self.offset = half, offset + half

    def end_halving(self, p):
        self.copies[p].wait()
        half, offset, start = self.length, self.offset - self.length, self.starts[-1]

        @pl.loop(0, half)
        def _(c):
            rows = self.part(start + c)
            self.acc[rows] = self.acc[rows] + self.recv[offset + c].astype(F32)

    def finish_own(self):
        start = self.starts[-1]
        self.full[start] = self.acc[self.part(start)].astype(BF16)

    def start_doubling(self, p):
        window = pl.ds(self.starts[p + 1], self.length)
        copy = remote(
            self.full.at[window],
            self.full.at[window],
            self.ag_send.at[p],
            self.ag_recv.at[p],
            "seq",
            self.peer(self.bits[p]),
        )
        copy.start()
        self.spread.append(copy)
        self.length *= 2

    def end_doubling(self):
        self.spread[-1].wait()


def kernel(
    n_seq, n_state, bits,
    x_ref, g_ref, b_ref, c_ref, rates_ref, ts_ref,
    gx_ref, in_full, out_full, gr_ref,
    gin_ref, gout_ref,
    xg, gg, gt, dec, tsb, dr, ad, bef, h_init, u_init, sh, ah, at,
    p_seg, u_seg, car, car2, rbuf, zs, zr,
    in_send, in_recv, out_send, out_recv,
    x_sems, g_sems, car_sems, car2_sems, rate_sems, z_sems, bar_sems, bar2_sems,
):
    tokens, feats = x_ref.shape
    chans = b_ref.shape[0]
    tiles, seg = chans // LANES, tokens // SEGMENTS
    seq, state = lax.axis_index("seq"), lax.axis_index("state")

    barrier = pltpu.get_barrier_semaphore()
    for k in range(1, n_seq):
        pl.semaphore_signal(
            barrier, inc=1, device_id={"seq": (seq + k) % n_seq}, device_id_type=MESH
        )
    for k in range(1, n_state):
        pl.semaphore_signal(
            barrier, inc=1, device_id={"state": (state + k) % n_state}, device_id_type=MESH
        )
    pl.semaphore_wait(barrier, n_seq + n_state - 2)

    def lanes(c):
        return slice(c * LANES, (c + 1) * LANES)

    tm = 256
    def columns(block):
        return pl.ds(multiple(block * feats, feats), feats)

    last = n_state - 1

    def hops(mine, held, sems, s):
        out = []
        for way, (block, go, source, here) in enumerate((
            (state - s, (state - s >= 0) & (state < last), state - 1 - s, state - 1 - s >= 0),
            (state + s, (state + s <= last) & (state > 0), state + 1 + s, state + 1 + s <= last),
        )):
            peer = state + 1 - 2 * way
            send = remote(
                mine if s == 0 else held.at[block], held.at[block],
                sems.at[0, way, s], sems.at[1, way, s], "state", peer,
            )
            arrive = remote(
                held.at[source], held.at[source],
                sems.at[0, way, s], sems.at[1, way, s], "state", state,
            )
            out.append((go, send, here, arrive, source))
        return out

    def send_step(steps):
        for go, send, _, _, _ in steps:
            pl.when(go)(send.start)

    def take_step(steps):
        for _, _, here, arrive, _ in steps:
            pl.when(here)(arrive.wait_recv)

    def use_step(steps, use):
        for _, _, here, _, source in steps:
            pl.when(here)(functools.partial(use, source))

    def drive_from(xb, block, fresh):
        @pl.loop(0, tokens // tm)
        def _(r):
            rows = pl.ds(multiple(r * tm, tm), tm)
            drive = lax.dot_general(
                xb[rows, :], b_ref[:, columns(block)], (((1,), (1,)), ((), ())),
                preferred_element_type=F32,
            )
            for c in range(tiles):
                dr[c, rows, :] = drive[:, lanes(c)] + (0.0 if fresh else dr[c, rows, :])

    def adjoint_from(gb, block, fresh):
        @pl.loop(0, tokens // tm)
        def _(r):
            rows = pl.ds(multiple(r * tm, tm), tm)
            back = jnp.dot(gb[rows, :], c_ref[columns(block), :], preferred_element_type=F32)
            for c in range(tiles):
                ad[c, rows, :] = back[:, lanes(c)] + (0.0 if fresh else ad[c, rows, :])
            gt[columns(block), rows] = gb[rows, :].T

    tm = 256
    x_steps = [hops(x_ref, xg, x_sems, s) for s in range(last)]
    g_steps = [hops(g_ref, gg, g_sems, s) for s in range(last)]
    use_x = lambda block: drive_from(xg.at[block], block, False)
    use_g = lambda block: adjoint_from(gg.at[block], block, False)
    for s in range(last):
        send_step(x_steps[s])
        if s == 0:

            @pl.loop(0, tokens // 64)
            def _(r):
                rows = pl.ds(multiple(r * 64, 64), 64)
                step = jnp.broadcast_to(ts_ref[rows, :], (64, LANES))
                tsb[rows, :] = step
                for c in range(tiles):
                    dec[c, rows, :] = jnp.exp(-step * rates_ref[:, lanes(c)])

            drive_from(x_ref, state, True)
        else:
            use_step(x_steps[s - 1], use_x)
        take_step(x_steps[s])
    send_step(g_steps[0])
    use_step(x_steps[last - 1], use_x)

    def strided(i):
        return pl.ds(i, SEGMENTS, stride=seg)

    zero = jnp.zeros((SEGMENTS, LANES), F32)
    one = jnp.ones((SEGMENTS, LANES), F32)

    def summarise(i, carry):
        hs, ps = [], []
        for c in range(tiles):
            a = dec[c, strided(i), :]
            hs.append(a * carry[0][c] + dr[c, strided(i), :])
            ps.append(a * carry[1][c])
        return tuple(hs), tuple(ps)

    def summarise_back(i, carry):
        j = seg - 1 - i
        return tuple(
            dec[c, strided(j), :] * (carry[c] + ad[c, strided(j), :]) for c in range(tiles)
        )

    def broadcast(buf, sems):
        copies = []
        for k in range(1, n_seq):
            copy = remote(
                buf.at[seq], buf.at[seq], sems.at[0, k], sems.at[1, k], "seq", (seq + k) % n_seq
            )
            copy.start()
            copies.append(copy)
        return copies

    def collect(buf, sems, copies):
        for k in range(1, n_seq):
            origin = (seq + n_seq - k) % n_seq
            remote(
                buf.at[origin], buf.at[origin], sems.at[0, k], sems.at[1, k], "seq", origin
            ).wait_recv()
        for copy in copies:
            copy.wait_send()

    hs, ps = lax.fori_loop(0, seg, summarise, ((zero,) * tiles, (one,) * tiles), unroll=4)
    for c in range(tiles):
        p, h = ps[c][0:1], hs[c][0:1]
        for k in range(1, SEGMENTS):
            h = ps[c][k : k + 1] * h + hs[c][k : k + 1]
            p = p * ps[c][k : k + 1]
        car[seq, 0:1, lanes(c)] = p
        car[seq, 1:2, lanes(c)] = h
        car[seq, 2:8, lanes(c)] = jnp.zeros((6, LANES), F32)
        p_seg[c] = ps[c]
    car_copies = broadcast(car, car_sems)
    adjoint_from(g_ref, state, True)
    collect(car, car_sems, car_copies)
    for c in range(tiles):
        h = jnp.zeros((1, LANES), F32)
        for k in range(n_seq - 1):
            new = car[k, 0:1, lanes(c)] * h + car[k, 1:2, lanes(c)]
            h = jnp.where(seq > k, new, h)
        for k in range(SEGMENTS):
            h_init[c, k : k + 1, :] = h
            h = ps[c][k : k + 1] * h + hs[c][k : k + 1]

    def sweep(i, carry):
        out = []
        for c in range(tiles):
            h = carry[c]
            bef[c, strided(i), :] = h
            h = dec[c, strided(i), :] * h + dr[c, strided(i), :]
            dr[c, strided(i), :] = h
            out.append(h)
        return tuple(out)

    lax.fori_loop(0, seg, sweep, tuple(h_init[c] for c in range(tiles)), unroll=4)

    @pl.loop(0, tokens // LANES)
    def _(r):
        rows = pl.ds(multiple(r * LANES, LANES), LANES)
        for c in range(tiles):
            sh[rows, lanes(c)] = dr[c, rows, :].astype(BF16)

    for s in range(last):
        take_step(g_steps[s])
        if s + 1 < last:
            send_step(g_steps[s + 1])
        use_step(g_steps[s], use_g)

    us = lax.fori_loop(0, seg, summarise_back, (zero,) * tiles, unroll=4)
    for c in range(tiles):
        u = us[c][SEGMENTS - 1 : SEGMENTS]
        for m in range(SEGMENTS - 2, -1, -1):
            u = p_seg[c, m : m + 1, :] * u + us[c][m : m + 1]
        car2[seq, :, lanes(c)] = jnp.broadcast_to(u, (SEGMENTS, LANES))
        u_seg[c] = us[c]
    car_copies = broadcast(car2, car2_sems)

    @pl.loop(0, gt.shape[0] // tm)
    def _(r):
        rows = pl.ds(multiple(r * tm, tm), tm)
        gout_ref[rows, :] = jnp.dot(gt[rows, :], sh[...], preferred_element_type=F32)

    swapped = bits[:1] + bits[:0:-1]
    second = Reducer(
        n_seq, swapped, gout_ref, out_send, out_recv, out_full, [bar2_sems.at[i] for i in range(4)]
    )
    second.start_halving(0)
    collect(car2, car2_sems, car_copies)
    for c in range(tiles):
        u = jnp.zeros((1, LANES), F32)
        for k in range(n_seq - 1, 0, -1):
            new = car[k, 0:1, lanes(c)] * u + car2[k, 0:1, lanes(c)]
            u = jnp.where(seq < k, new, u)
        for m in range(SEGMENTS - 1, -1, -1):
            u_init[c, m : m + 1, :] = u
            u = p_seg[c, m : m + 1, :] * u + u_seg[c, m : m + 1, :]

    def sweep_back(i, carry):
        us, rs = [], []
        j = seg - 1 - i
        step = tsb[strided(j), :]
        for c in range(tiles):
            adj = ad[c, strided(j), :] + carry[0][c]
            ad[c, strided(j), :] = adj
            u = dec[c, strided(j), :] * adj
            us.append(u)
            rs.append(carry[1][c] + step * u * bef[c, strided(j), :])
        return tuple(us), tuple(rs)

    _, rs = lax.fori_loop(
        0, seg, sweep_back,
        (tuple(u_init[c] for c in range(tiles)), (zero,) * tiles),
        unroll=4,
    )
    for c in range(tiles):
        rbuf[seq, :, lanes(c)] = jnp.broadcast_to(
            -jnp.sum(rs[c], axis=0, keepdims=True), (SEGMENTS, LANES)
        )
    rate_copies = broadcast(rbuf, rate_sems)

    @pl.loop(0, tokens // LANES)
    def _(r):
        rows = pl.ds(multiple(r * LANES, LANES), LANES)
        for c in range(tiles):
            half = ad[c, rows, :].astype(BF16)
            ah[rows, lanes(c)] = half
            at[lanes(c), rows] = half.T

    def input_terms(k):
        cols = pl.ds(multiple(((state + k) % n_state) * feats, feats), feats)

        @pl.loop(0, tokens // tm)
        def _(r):
            rows = pl.ds(multiple(r * tm, tm), tm)
            zs[k, rows, :] = jnp.dot(
                ah[rows, :], b_ref[:, cols], preferred_element_type=F32
            ).astype(BF16)

    z_copies = []
    for k in range(1, n_state):
        input_terms(k)
        copy = remote(
            zs.at[k], zr.at[k], z_sems.at[0, k], z_sems.at[1, k], "state", (state + k) % n_state
        )
        copy.start()
        z_copies.append(copy)

    second.end_halving(0)
    second.start_halving(1)

    def gin_from(xb, block):
        tc = min(tm, chans)

        @pl.loop(0, chans // tc)
        def _(r):
            rows = pl.ds(multiple(r * tc, tc), tc)
            gin_ref[rows, columns(block)] = jnp.dot(at[rows, :], xb[...], preferred_element_type=F32)

    gin_from(x_ref, state)
    for k in range(1, n_state):
        other = (state + k) % n_state
        gin_from(xg.at[other], other)

    first = Reducer(
        n_seq, bits, gin_ref, in_send, in_recv, in_full, [bar_sems.at[i] for i in range(4)]
    )
    first.start_halving(0)
    both = (second, first)
    input_terms(0)
    for p in range(len(bits)):
        for red in both:
            if red is second and p == 0:
                continue
            red.end_halving(p)
            if p + 1 < len(bits):
                red.start_halving(p + 1)
            else:
                red.finish_own()
                red.start_doubling(p)
    for p in range(len(bits) - 2, -1, -1):
        for red in both:
            red.end_doubling()
            red.start_doubling(p)
        if p == min(1, len(bits) - 2):
            collect(rbuf, rate_sems, rate_copies)
            total = rbuf[0, 0:1, :]
            for k in range(1, n_seq):
                total = total + rbuf[k, 0:1, :]
            gr_ref[...] = total
            for copy in z_copies:
                copy.wait()

            @pl.loop(0, tokens // 64)
            def _(r):
                rows = pl.ds(multiple(r * 64, 64), 64)
                terms = zs[0, rows, :].astype(F32)
                for k in range(1, n_state):
                    terms = terms + zr[k, rows, :].astype(F32)
                gx_ref[rows, :] = terms.astype(BF16)

    for red in both:
        red.end_doubling()
    for step in x_steps + g_steps:
        for go, send, _, _, _ in step:
            pl.when(go)(send.wait_send)


def on_device(inputs, out_grad, in_proj, out_proj, rates, time_step):
    n_seq, n_state = lax.axis_size("seq"), lax.axis_size("state")
    tokens, feats = inputs.shape
    chans, width = in_proj.shape
    tiles = chans // LANES
    bits = list(range(n_seq.bit_length() - 1))
    vmem = pltpu.VMEM
    dma = pltpu.SemaphoreType.DMA
    tile = vmem((tiles, tokens, LANES), F32)
    down = min(n_seq, chans // 16)
    in_shape = (n_seq, chans // down, width * down // n_seq)
    out_shape = (n_seq, width // n_seq, chans)
    in_part, out_part = vmem(in_shape, BF16), vmem(out_shape, BF16)
    seg_part = vmem((tiles, SEGMENTS, LANES), F32)
    carries = vmem((n_seq, SEGMENTS, chans), F32)
    whole = pl.BlockSpec(memory_space=pltpu.VMEM)
    gx, gin, gout, gr = pl.pallas_call(
        functools.partial(kernel, n_seq, n_state, bits),
        out_shape=(
            jax.ShapeDtypeStruct((tokens, feats), BF16),
            jax.ShapeDtypeStruct(in_shape, BF16),
            jax.ShapeDtypeStruct(out_shape, BF16),
            jax.ShapeDtypeStruct((1, chans), F32),
        ),
        in_specs=[whole] * 6,
        out_specs=(whole,) * 4,
        scratch_shapes=[
            vmem((chans, width), F32),
            vmem((width, chans), F32),
            vmem((n_state, tokens, feats), BF16),
            vmem((n_state, tokens, feats), BF16),
            vmem((width, tokens), BF16),
            tile,
            vmem((tokens, LANES), F32),
            tile, tile, tile,
            seg_part, seg_part,
            vmem((tokens, chans), BF16),
            vmem((tokens, chans), BF16),
            vmem((chans, tokens), BF16),
            seg_part, seg_part,
            carries, carries, carries,
            vmem((n_state, tokens, feats), BF16),
            vmem((n_state, tokens, feats), BF16),
            in_part, in_part, out_part, out_part,
            dma((2, 2, n_state)),
            dma((2, 2, n_state)),
            dma((2, n_seq)),
            dma((2, n_seq)),
            dma((2, n_seq)),
            dma((2, n_state)),
            dma((4, len(bits))),
            dma((4, len(bits))),
        ],
        compiler_params=pltpu.CompilerParams(
            collective_id=0, has_side_effects=True, vmem_limit_bytes=60 * 1024 * 1024
        ),
    )(
        inputs, out_grad, in_proj, out_proj,
        rates.reshape(1, chans), time_step.reshape(tokens, 1),
    )
    gin = gin.reshape(down, n_seq // down, *in_shape[1:]).transpose(0, 2, 1, 3)
    gin = gin.reshape(chans, width).astype(F32)
    gout = gout.reshape(width, chans).astype(F32)
    return gx, gin, gout, gr.reshape(chans)


def solution(mesh):
    placed = (
        P("seq", "state"),
        P("seq", "state"),
        P("state", None),
        P(None, "state"),
        P("state"),
        P("seq"),
    )
    return jax.shard_map(
        on_device,
        mesh=mesh,
        in_specs=placed,
        out_specs=(P("seq", "state"), P("state", None), P(None, "state"), P("state")),
        check_vma=False,
    )
```
